32 devices in a mesh: row: 8 (over z, y), col: 4 (over x, core).
Axes of the slice: x: 2, y: 2, z: 4, core: 2. Of those that a mesh axis runs over, the one named last changes fastest.
Arguments:
- dens_alpha: bfloat16 [2048, 2048], P('row', 'col'), may hold values from -6 to 6
- dens_beta: bfloat16 [2048, 2048], P('row', 'col'), may hold values from -6 to 6
- integrals: bfloat16 [512, 256, 256], P(('row', 'col')), may hold values from -0.375 to 0.375
- tile_quartet: int32 [512, 4], P(('row', 'col')), may hold values from 0 to 127, as said below
- tile_count: int32 [32], P(('row', 'col')), may hold values from 2 to 16, as said below
Outputs:
- fock_alpha: float32 [2048, 2048], P('row', 'col')
- fock_beta: float32 [2048, 2048], P('row', 'col')
The draws below stay inside these ranges and needn't reach their ends.
Inputs may be any that keep to these rules, and one draw needn't show every extreme that they name: `tile_quartet`: slots d * 16 to d * 16 + 15 belong to device d = i * 4 + j (i its row index, j its col index). Each row holds block indices P, Q, R, S of 16 functions; Q lies in i * 16 up to but excluding (i + 1) * 16, and R in j * 32 up to but excluding (j + 1) * 32; S may be any block. Among the 16 slots of one device, exactly 2 have P in each range k * 16 up to but excluding (k + 1) * 16, and so exactly 4 in each range of width 2048 // 64; their order within the device is arbitrary. `tile_count`: the live slots of a device are its first ones; some device has all 16 live.
All inputs are finite; a program needn't handle non-finite values.
Results may differ from the reference program's by a relative error of at most 0.0026.
Values may be sent and summed in bfloat16 or wider, within the bound.
A program may use at most 128 MiB of HBM per device.

```python
import jax
import jax.numpy as jnp
from jax import lax

NBASIS = 2048
SHELL = 16
SLOTS = 16
TILES = 512
N_ROW = 8
N_COL = 4


def draw_tile_count(key, part):
    device_total = N_ROW * N_COL
    key_div, key_full = jax.random.split(jax.random.fold_in(key, 11))
    divisor = jax.random.randint(key_div, (device_total,), 1, 9)
    counts = SLOTS // divisor
    full_device = jax.random.randint(key_full, (), 0, device_total)
    return jnp.where(jnp.arange(device_total) == full_device, SLOTS, counts).astype(jnp.int32)


def draw_tile_quartet(key, part):
    keys = jax.random.split(jax.random.fold_in(key, 23), 7)
    device_total = N_ROW * N_COL
    total = device_total * SLOTS
    device = jnp.arange(total, dtype=jnp.int32) // SLOTS
    row_blocks = NBASIS // (N_ROW * SHELL)
    col_blocks = NBASIS // (N_COL * SHELL)
    all_blocks = NBASIS // SHELL
    ratio = N_ROW // N_COL
    base = jnp.broadcast_to(jnp.arange(SLOTS, dtype=jnp.int32)[None, :], (device_total, SLOTS))
    shuffled = jax.random.permutation(keys[4], base, axis=1, independent=True).reshape(total)
    offset_col = jax.random.randint(keys[5], (device_total,), 0, N_COL)[device]
    offset_sub = jax.random.randint(keys[6], (device_total,), 0, ratio)[device]
    dest_col = (shuffled + offset_col) % N_COL
    dest_sub = (shuffled // N_COL + offset_sub) % ratio
    dest_row = dest_col * ratio + dest_sub
    index_p = dest_row * row_blocks + jax.random.randint(keys[0], (total,), 0, row_blocks)
    index_q = device // N_COL * row_blocks + jax.random.randint(keys[1], (total,), 0, row_blocks)
    index_r = device % N_COL * col_blocks + jax.random.randint(keys[2], (total,), 0, col_blocks)
    index_s = jax.random.randint(keys[3], (total,), 0, all_blocks)
    return jnp.stack([index_p, index_q, index_r, index_s], 1).astype(jnp.int32)


def shard_levels(key, shape, shards, low, high):
    level = 1.0
    for position, parts in shards:
        steps = jax.random.uniform(jax.random.fold_in(jax.random.fold_in(key, 6), position), (parts,), jnp.float32, low / len(shards), high / len(shards))
        level = level * jnp.repeat(jnp.exp(steps), shape[position] // parts).reshape((-1,) + (1,) * (len(shape) - 1 - position))
    return level


def centred(own_key, shape, scale, most, shards=(), held_as=jnp.bfloat16):
    gain = shard_levels(own_key, shape, shards, -0.22, 0.18) if shards else 1.0
    entries = jax.random.normal(own_key, shape, jnp.float32) * scale * gain
    return jnp.minimum(jnp.maximum(entries, -most), most).astype(held_as)


def setup_inputs(seed: int = 0) -> dict:
    key_list = jax.random.split(jax.random.key(seed), 6)
    return {
        "dens_alpha": centred(key_list[0], (NBASIS, NBASIS), 1.0, 6.0, ((0, 8), (1, 4))),
        "dens_beta": centred(key_list[1], (NBASIS, NBASIS), 1.0, 6.0, ((0, 8), (1, 4))),
        "integrals": centred(key_list[2], (TILES, SHELL * SHELL, SHELL * SHELL), (SHELL * SHELL) ** -0.5, 0.375, ((0, 32),)),
        "tile_quartet": draw_tile_quartet(jax.random.fold_in(key_list[5], 71), 0),
        "tile_count": draw_tile_count(jax.random.fold_in(key_list[5], 71), 0),
    }


def reference(dens_alpha, dens_beta, integrals, tile_quartet, tile_count):
    block_count = NBASIS // SHELL
    summed = (dens_alpha.astype(jnp.float32) + dens_beta.astype(jnp.float32)).astype(jnp.bfloat16)
    summed_view = summed.reshape(block_count, SHELL, block_count, SHELL)
    alpha_view = dens_alpha.reshape(block_count, SHELL, block_count, SHELL)
    beta_view = dens_beta.reshape(block_count, SHELL, block_count, SHELL)
    offsets = jnp.arange(SHELL, dtype=jnp.int32)

    def visit(totals, device):
        coulomb, exch_alpha, exch_beta = totals
        first_slot = (device * SLOTS).astype(jnp.int32)
        tile_data = lax.dynamic_slice_in_dim(integrals, first_slot, SLOTS, 0).astype(jnp.float32)
        tile_data = tile_data.reshape(SLOTS, SHELL, SHELL, SHELL, SHELL)
        quartets = lax.dynamic_slice_in_dim(tile_quartet, first_slot, SLOTS, 0)
        index_p = quartets[:, 0]
        index_q = quartets[:, 1]
        index_r = quartets[:, 2]
        index_s = quartets[:, 3]
        live_mask = (jnp.arange(SLOTS, dtype=jnp.int32) < tile_count[device]).astype(jnp.float32)[:, None, None]
        coul_dens = summed_view[index_s, :, index_r, :].astype(jnp.float32)
        alpha_dens = alpha_view[index_q, :, index_s, :].astype(jnp.float32)
        beta_dens = beta_view[index_q, :, index_s, :].astype(jnp.float32)
        coul_part = jnp.einsum('tpqrs,tsr->tqp', tile_data, coul_dens) * live_mask
        alpha_part = jnp.einsum('tpqrs,tqs->tpr', tile_data, alpha_dens) * live_mask
        beta_part = jnp.einsum('tpqrs,tqs->tpr', tile_data, beta_dens) * live_mask
        rows_q = index_q[:, None, None] * SHELL + offsets[None, :, None]
        cols_p = index_p[:, None, None] * SHELL + offsets[None, None, :]
        coulomb = coulomb.at[rows_q, cols_p].add(coul_part)
        rows_p = index_p[:, None, None] * SHELL + offsets[None, :, None]
        cols_r = index_r[:, None, None] * SHELL + offsets[None, None, :]
        exch_alpha = exch_alpha.at[rows_p, cols_r].add(alpha_part)
        exch_beta = exch_beta.at[rows_p, cols_r].add(beta_part)
        return (coulomb, exch_alpha, exch_beta), None

    empty_fock = jnp.zeros((NBASIS, NBASIS), jnp.float32)
    devices = jnp.arange(N_ROW * N_COL, dtype=jnp.int32)
    (coulomb, exch_alpha, exch_beta), unused = lax.scan(visit, (empty_fock, empty_fock, empty_fock), devices)
    return coulomb - exch_alpha, coulomb - exch_beta
```

```python
import functools

import jax
import jax.numpy as jnp
from jax import lax
from jax.experimental import pallas as pl
from jax.experimental.pallas import tpu as pltpu
from jax.sharding import PartitionSpec as P

SHELL = 16
LANES = 128
PACK = LANES // SHELL
WORDS = 8
MESH = pl.DeviceIdType.MESH
F32 = jnp.float32
BF16 = jnp.bfloat16


def iota(shape, axis):
    return lax.broadcasted_iota(jnp.int32, shape, axis)


def one_hot(shape, test):
    return jnp.where(test(iota(shape, 0), iota(shape, 1)), 1.0, 0.0).astype(BF16)


def dot(left, right):
    return jnp.dot(left, right, preferred_element_type=F32)


def dot_split(value, right):
    high = value.astype(BF16)
    low = (value - high.astype(F32)).astype(BF16)
    return dot(high, right) + dot(low, right)


def build_kernel(
    n_row, n_col, quartet, count, dens_a, dens_b, tiles,
    out_x, out_c, place,
    meta_c, meta_r, split_a, split_b, summed, held, send_c, recv_c, send_r, recv_r,
    drep_a, drep_b, left_j, part_a, part_b, part_j,
    xs, xr, cs, cr,
    tile_sem, sems_c, semr_c, sems_r, semr_r,
):
    slots, width = tiles.shape[0], tiles.shape[1]
    row_blocks = dens_a.shape[0] // SHELL
    col_blocks = dens_a.shape[1] // SHELL
    chunks = col_blocks // PACK
    row_cap, col_cap = slots // n_row, slots // n_col
    my_row, my_col = lax.axis_index("row"), lax.axis_index("col")
    first_row, first_col = my_row * row_blocks, my_col * col_blocks

    def row_peer(step):
        return lax.rem(my_row + step, n_row)

    def col_peer(step):
        return lax.rem(my_col + step, n_col)

    def column_copy(kind, src, dst, peer, source):
        return pltpu.make_async_remote_copy(
            src_ref=src, dst_ref=dst,
            send_sem=sems_c.at[kind, peer], recv_sem=semr_c.at[kind, source],
            device_id=(peer, my_col), device_id_type=MESH,
        )

    def row_copy(kind, src, dst, peer, source):
        return pltpu.make_async_remote_copy(
            src_ref=src, dst_ref=dst,
            send_sem=sems_r.at[kind, peer], recv_sem=semr_r.at[kind, source],
            device_id=(my_row, peer), device_id_type=MESH,
        )

    barrier = pltpu.get_barrier_semaphore()
    for step in range(1, n_row):
        pl.semaphore_signal(
            barrier, inc=1, device_id=(row_peer(step), my_col), device_id_type=MESH
        )
    for step in range(1, n_col):
        pl.semaphore_signal(
            barrier, inc=1, device_id=(my_row, col_peer(step)), device_id_type=MESH
        )
    pieces = tile_sem.shape[0]
    piece = slots // pieces
    tile_copies = [
        pltpu.make_async_copy(
            tiles.at[pl.ds(n * piece, piece)], held.at[pl.ds(n * piece, piece)], tile_sem.at[n]
        )
        for n in range(pieces)
    ]
    for copy in tile_copies:
        copy.start()

    live_count = count[0]
    keys = [lax.div(quartet[t, 0], row_blocks) * slots + t for t in range(slots)]

    def pick(u, previous):
        found = [jnp.where(key > previous, key, 1 << 30) for key in keys]
        while len(found) > 1:
            found = [jnp.minimum(a, b) for a, b in zip(found[::2], found[1::2])]
        t = lax.rem(found[0], slots)
        words = [quartet[t, n] for n in range(4)] + [jnp.where(t < live_count, 1, 0), t]
        for n, word in enumerate(words):
            meta_c[my_row, u * WORDS + n] = word
            meta_r[my_col, u * WORDS + n] = word
        return found[0]

    lax.fori_loop(0, slots, pick, jnp.int32(-1))
    for block_row in range(row_blocks):
        for chunk in range(chunks):
            rows = slice(block_row * SHELL, (block_row + 1) * SHELL)
            lanes = slice(chunk * LANES, (chunk + 1) * LANES)
            alpha, beta = dens_a[rows, lanes], dens_b[rows, lanes]
            at = block_row * chunks + chunk
            split_a[at], split_b[at] = alpha, beta
            summed[at] = (alpha.astype(F32) + beta.astype(F32)).astype(BF16)

    pl.semaphore_wait(barrier, n_row + n_col - 2)
    for step in range(n_row - 1, 0, -1):
        column_copy(0, meta_c.at[my_row], meta_c.at[my_row], row_peer(step), my_row).start()
    for step in range(1, n_col):
        row_copy(0, meta_r.at[my_col], meta_r.at[my_col], col_peer(step), my_col).start()

    group = iota((SHELL, LANES), 1) // SHELL

    fold_one = one_hot((LANES, LANES), lambda i, j: lax.rem(i, SHELL) == lax.rem(j, SHELL))

    def block_of(ref, block_row, block_col, mine):
        chunk = ref[block_row * chunks + lax.div(block_col, PACK)].astype(F32)
        inside = jnp.where(mine, lax.rem(block_col, PACK), -1)
        return jnp.where(group == inside, chunk, 0.0)

    def packed_blocks(blocks):
        spread_out = dot(jnp.concatenate(blocks, axis=0).astype(BF16), fold_one)
        halves = []
        for half in range(slots // PACK):
            total = jnp.zeros((SHELL, LANES), F32)
            for slot in range(PACK):
                first = (half * PACK + slot) * SHELL
                total = jnp.where(group == slot, spread_out[first : first + SHELL], total)
            halves.append(total)
        return jnp.concatenate(halves, axis=0).astype(BF16)

    def answer_column(source, target):
        blocks = []
        for slot in range(slots):
            s_at = meta_c[source, slot * WORDS + 3] - first_row
            r_at = jnp.clip(meta_c[source, slot * WORDS + 2] - first_col, 0, col_blocks - 1)
            mine = (s_at >= 0) & (s_at < row_blocks)
            blocks.append(block_of(summed, jnp.where(mine, s_at, 0), r_at, mine))
        target[source] = packed_blocks(blocks)

    def answer_row(source, target):
        blocks = [[], []]
        for slot in range(slots):
            q_at = jnp.clip(meta_r[source, slot * WORDS + 1] - first_row, 0, row_blocks - 1)
            s_at = meta_r[source, slot * WORDS + 3] - first_col
            mine = (s_at >= 0) & (s_at < col_blocks)
            s_at = jnp.where(mine, s_at, 0)
            for x, ref in enumerate((split_a, split_b)):
                blocks[x].append(block_of(ref, q_at, s_at, mine))
        half_rows = slots // PACK * SHELL
        for x in range(2):
            target[source, x * half_rows : (x + 1) * half_rows, :] = packed_blocks(blocks[x])

    answer_column(my_row, recv_c)
    answer_row(my_col, recv_r)

    def serve_row(step, carry):
        peer = col_peer(step)
        row_copy(0, meta_r.at[peer], meta_r.at[peer], peer, peer).wait_recv()
        answer_row(peer, send_r)
        row_copy(1, send_r.at[peer], recv_r.at[my_col], peer, my_col).start()
        return carry

    def serve_column(step, carry):
        peer = row_peer(step)
        column_copy(0, meta_c.at[peer], meta_c.at[peer], peer, peer).wait_recv()
        answer_column(peer, send_c)
        column_copy(1, send_c.at[peer], recv_c.at[my_row], peer, my_row).start()
        return carry

    lax.fori_loop(1, n_col, serve_row, 0)
    lax.fori_loop(1, n_row, serve_column, 0)

    def place_row(source, carry):
        for m in range(row_cap):
            base = (my_row * row_cap + m) * WORDS
            at = (source * row_cap + m) * 4
            place[at] = meta_c[source, base] - first_row
            place[at + 1] = meta_c[source, base + 2] - first_col
            place[at + 2] = meta_c[source, base + 4]
        return carry

    def place_col(source, carry):
        for m in range(col_cap):
            base = (my_col * col_cap + m) * WORDS
            at = (slots + source * col_cap + m) * 4
            place[at] = meta_r[source, base + 1] - first_row
            place[at + 1] = meta_r[source, base] - first_col
            place[at + 2] = meta_r[source, base + 4]
        return carry

    lax.fori_loop(0, n_row, place_row, 0)
    lax.fori_loop(0, n_col, place_col, 0)

    fold = one_hot((LANES, width), lambda i, j: lax.rem(i, SHELL) == lax.rem(j, SHELL))
    spread = one_hot((LANES, width), lambda i, j: lax.rem(i, SHELL) == lax.div(j, SHELL))
    gather = one_hot((width, LANES), lambda i, j: lax.div(i, SHELL) == lax.rem(j, SHELL))
    total_rows = slots * SHELL
    same_slot = one_hot(
        (total_rows, total_rows), lambda i, j: lax.div(i, SHELL) == lax.div(j, SHELL)
    )
    shape = (total_rows, width)
    diagonal = lax.rem(iota(shape, 0), SHELL) == lax.rem(iota(shape, 1), SHELL)

    def expand(packed):
        return jnp.concatenate(
            [
                jnp.where(
                    group == t % PACK,
                    packed[(t // PACK) * SHELL : (t // PACK + 1) * SHELL],
                    0.0,
                )
                for t in range(slots)
            ],
            axis=0,
        ).astype(BF16)

    def arrive(count_of, copy_of, peer_of, ref):
        def wait(step, carry):
            copy_of(1, ref.at[peer_of(step)], ref.at[peer_of(step)], peer_of(step), peer_of(step)).wait_recv()
            return carry

        lax.fori_loop(1, count_of, wait, 0)
        total = ref[0].astype(F32)
        for n in range(1, count_of):
            total = total + ref[n].astype(F32)
        return total

    spins = arrive(n_col, row_copy, col_peer, recv_r)
    half_rows = (slots // PACK) * SHELL
    drep_a[...] = dot(expand(spins[:half_rows]), fold)
    drep_b[...] = dot(expand(spins[half_rows:]), fold)
    for copy in tile_copies:
        copy.wait()

    def exchange(t, carry):
        rows = pl.ds(pl.multiple_of(t * SHELL, SHELL), SHELL)
        tile = held[meta_c[my_row, t * WORDS + 5]].astype(F32).reshape(SHELL, SHELL, width)
        part_a[rows, :] = jnp.sum(tile * drep_a[rows, :][None], axis=1)
        part_b[rows, :] = jnp.sum(tile * drep_b[rows, :][None], axis=1)
        return carry

    lax.fori_loop(0, slots, exchange, 0)
    exch_a = dot_split(part_a[...], gather)
    exch_b = dot_split(part_b[...], gather)
    for k in range(n_row):
        total = jnp.zeros((SHELL, LANES), F32)
        for m in range(row_cap):
            first = (k * row_cap + m) * SHELL
            total = jnp.where(group == 2 * m, exch_a[first : first + SHELL], total)
            total = jnp.where(group == 2 * m + 1, exch_b[first : first + SHELL], total)
        xs[k] = total

    def send_x(step, carry):
        peer = row_peer(step)
        column_copy(2, xs.at[peer], xr.at[my_row], peer, my_row).start()
        return carry

    lax.fori_loop(1, n_row, send_x, 0)
    xr[my_row] = xs[my_row]

    coul = arrive(n_row, column_copy, row_peer, recv_c)
    left_j[...] = dot(
        same_slot, jnp.where(diagonal, dot(expand(coul), spread), 0.0).astype(BF16)
    ).astype(BF16)

    def coulomb(t, carry):
        rows = pl.ds(pl.multiple_of(t * SHELL, SHELL), SHELL)
        part_j[rows, :] = lax.dot_general(
            left_j[rows, :], held[meta_c[my_row, t * WORDS + 5]], (((1,), (1,)), ((), ())), preferred_element_type=F32
        )
        return carry

    lax.fori_loop(0, slots, coulomb, 0)
    coul_blocks = dot_split(jnp.where(diagonal, part_j[...], 0.0), gather)
    for k in range(n_col):
        total = jnp.zeros((SHELL, LANES), F32)
        for m in range(col_cap):
            first = (k * col_cap + m) * SHELL
            total = jnp.where(group == m, coul_blocks[first : first + SHELL], total)
        cs[k] = total

    def send_j(step, carry):
        peer = col_peer(step)
        row_copy(2, cs.at[peer], cr.at[my_col], peer, my_col).start()
        return carry

    lax.fori_loop(1, n_col, send_j, 0)
    cr[my_col] = cs[my_col]

    def finish_row(step, carry):
        peer = col_peer(step)
        row_copy(2, cs.at[peer], cr.at[peer], peer, peer).wait()
        row_copy(1, send_r.at[peer], recv_r.at[peer], peer, peer).wait_send()
        row_copy(0, meta_r.at[my_col], meta_r.at[my_col], peer, peer).wait_send()
        return carry

    def finish_column(step, carry):
        peer = row_peer(step)
        column_copy(2, xs.at[peer], xr.at[peer], peer, peer).wait()
        column_copy(1, send_c.at[peer], recv_c.at[peer], peer, peer).wait_send()
        column_copy(0, meta_c.at[my_row], meta_c.at[my_row], peer, peer).wait_send()
        return carry

    lax.fori_loop(1, n_row, finish_column, 0)
    lax.fori_loop(1, n_col, finish_row, 0)
    out_x[...] = xr[...]
    out_c[...] = cr[...]


def place_kernel(place, in_x, in_c, out_a, out_b):
    n_row, n_col = in_x.shape[0], in_c.shape[0]
    slots = place.shape[0] // 8
    row_cap, col_cap = slots // n_row, slots // n_col
    out_a[...] = jnp.zeros_like(out_a)
    out_b[...] = jnp.zeros_like(out_b)
    group = iota((SHELL, LANES), 1) // SHELL

    def where_to(at):
        block_col = place[at + 1]
        rows = pl.ds(pl.multiple_of(place[at] * SHELL, SHELL), SHELL)
        lanes = pl.ds(pl.multiple_of(lax.div(block_col, PACK) * LANES, LANES), LANES)
        inside = lax.rem(block_col, PACK)
        return rows, lanes, inside, group == jnp.where(place[at + 2] != 0, inside, -1)

    def moved(block, here, inside, mask):
        shift = lax.rem(inside - here + PACK, PACK) * SHELL
        return jnp.where(mask, pltpu.roll(block, shift, 1), 0.0)

    for source in range(n_col):
        block = in_c[source]
        for m in range(col_cap):
            rows, lanes, inside, mask = where_to((slots + source * col_cap + m) * 4)
            value = moved(block, m, inside, mask)
            out_a[rows, lanes] += value
            out_b[rows, lanes] += value
    for source in range(n_row):
        block = in_x[source]
        for m in range(row_cap):
            rows, lanes, inside, mask = where_to((source * row_cap + m) * 4)
            out_a[rows, lanes] -= moved(block, 2 * m, inside, mask)
            out_b[rows, lanes] -= moved(block, 2 * m + 1, inside, mask)


def local(n_row, n_col, dens_alpha, dens_beta, integrals, tile_quartet, tile_count):
    slots, width = integrals.shape[0], integrals.shape[1]
    vmem = pl.BlockSpec(memory_space=pltpu.VMEM)
    smem = pl.BlockSpec(memory_space=pltpu.SMEM)
    rows = slots * SHELL
    pack_rows = slots // PACK * SHELL
    meta_words = max(LANES, slots * WORDS)
    split = pltpu.VMEM((dens_alpha.size // (SHELL * LANES), SHELL, LANES), BF16)
    blocks_x, blocks_c, place = pl.pallas_call(
        functools.partial(build_kernel, n_row, n_col),
        out_shape=(
            jax.ShapeDtypeStruct((n_row, SHELL, LANES), F32),
            jax.ShapeDtypeStruct((n_col, SHELL, LANES), F32),
            jax.ShapeDtypeStruct((slots * 8,), jnp.int32),
        ),
        in_specs=[smem, smem, vmem, vmem, pl.BlockSpec(memory_space=pl.ANY)],
        out_specs=(vmem, vmem, smem),
        scratch_shapes=[
            pltpu.SMEM((n_row, meta_words), jnp.int32),
            pltpu.SMEM((n_col, meta_words), jnp.int32),
            split,
            split,
            split,
            pltpu.VMEM(integrals.shape, BF16),
            pltpu.VMEM((n_row, pack_rows, LANES), BF16),
            pltpu.VMEM((n_row, pack_rows, LANES), BF16),
            pltpu.VMEM((n_col, 2 * pack_rows, LANES), BF16),
            pltpu.VMEM((n_col, 2 * pack_rows, LANES), BF16),
            pltpu.VMEM((rows, width), F32),
            pltpu.VMEM((rows, width), F32),
            pltpu.VMEM((rows, width), BF16),
            pltpu.VMEM((rows, width), F32),
            pltpu.VMEM((rows, width), F32),
            pltpu.VMEM((rows, width), F32),
            pltpu.VMEM((n_row, SHELL, LANES), F32),
            pltpu.VMEM((n_row, SHELL, LANES), F32),
            pltpu.VMEM((n_col, SHELL, LANES), F32),
            pltpu.VMEM((n_col, SHELL, LANES), F32),
            pltpu.SemaphoreType.DMA((4,)),
            pltpu.SemaphoreType.DMA((3, n_row)),
            pltpu.SemaphoreType.DMA((3, n_row)),
            pltpu.SemaphoreType.DMA((3, n_col)),
            pltpu.SemaphoreType.DMA((3, n_col)),
        ],
        compiler_params=pltpu.CompilerParams(collective_id=0, has_side_effects=True),
        name="build",
    )(tile_quartet, tile_count, dens_alpha, dens_beta, integrals)
    out = jax.ShapeDtypeStruct(dens_alpha.shape, F32)
    return pl.pallas_call(
        place_kernel,
        out_shape=(out, out),
        in_specs=[smem, vmem, vmem],
        out_specs=(vmem, vmem),
        name="place",
    )(place, blocks_x, blocks_c)


def solution(mesh):
    in_specs = (
        P("row", "col"),
        P("row", "col"),
        P(("row", "col"), None, None),
        P(("row", "col"), None),
        P(("row", "col")),
    )
    body = functools.partial(local, mesh.shape["row"], mesh.shape["col"])
    return jax.shard_map(
        body, mesh=mesh, in_specs=in_specs, out_specs=(P("row", "col"), P("row", "col")),
        check_vma=False,
    )
```

```python
import functools

import jax
import jax.numpy as jnp
from jax import lax
from jax.experimental import pallas as pl
from jax.experimental.pallas import tpu as pltpu
from jax.sharding import PartitionSpec as P

SHELL = 16
LANES = 128
PACK = LANES // SHELL
WORDS = 8
MESH = pl.DeviceIdType.MESH
F32 = jnp.float32
BF16 = jnp.bfloat16


def iota(shape, axis):
    return lax.broadcasted_iota(jnp.int32, shape, axis)


def one_hot(shape, test):
    return jnp.where(test(iota(shape, 0), iota(shape, 1)), 1.0, 0.0).astype(BF16)


def dot(left, right):
    return jnp.dot(left, right, preferred_element_type=F32)


def dot_split(value, right):
    high = value.astype(BF16)
    low = (value - high.astype(F32)).astype(BF16)
    return dot(high, right) + dot(low, right)


def build_kernel(
    n_row, n_col, hbm_quartet, hbm_count, hbm_a, hbm_b, tiles,
    out_x, out_c, place,
    quartet, count, dens_a, dens_b, meta_c, meta_r, split_a, split_b, summed, held, send_c, recv_c, send_r, recv_r,
    drep_a, drep_b, weights, part_a, part_b, blocks_j,
    xs, xr, cs, cr,
    index_sem, dens_sem, tile_sem, sems_c, semr_c, sems_r, semr_r,
):
    slots, width = tiles.shape[0], tiles.shape[1]
    row_blocks = hbm_a.shape[0] // SHELL
    col_blocks = hbm_a.shape[1] // SHELL
    chunks = col_blocks // PACK
    row_cap, col_cap = slots // n_row, slots // n_col
    my_row, my_col = lax.axis_index("row"), lax.axis_index("col")
    first_row, first_col = my_row * row_blocks, my_col * col_blocks

    def row_peer(step):
        return lax.rem(my_row + step, n_row)

    def col_peer(step):
        return lax.rem(my_col + step, n_col)

    def column_copy(kind, src, dst, peer, source):
        return pltpu.make_async_remote_copy(
            src_ref=src, dst_ref=dst,
            send_sem=sems_c.at[kind, peer], recv_sem=semr_c.at[kind, source],
            device_id=(peer, my_col), device_id_type=MESH,
        )

    def row_copy(kind, src, dst, peer, source):
        return pltpu.make_async_remote_copy(
            src_ref=src, dst_ref=dst,
            send_sem=sems_r.at[kind, peer], recv_sem=semr_r.at[kind, source],
            device_id=(my_row, peer), device_id_type=MESH,
        )

    index_copies = [
        pltpu.make_async_copy(src, dst, index_sem.at[n])
        for n, (src, dst) in enumerate(((hbm_quartet, quartet), (hbm_count, count)))
    ]
    for copy in index_copies:
        copy.start()
    dens_copies = [
        pltpu.make_async_copy(src, dst, dens_sem.at[n])
        for n, (src, dst) in enumerate(((hbm_a, dens_a), (hbm_b, dens_b)))
    ]
    for copy in dens_copies:
        copy.start()
    barrier = pltpu.get_barrier_semaphore()
    for step in range(1, n_row):
        pl.semaphore_signal(
            barrier, inc=1, device_id=(row_peer(step), my_col), device_id_type=MESH
        )
    for step in range(1, n_col):
        pl.semaphore_signal(
            barrier, inc=1, device_id=(my_row, col_peer(step)), device_id_type=MESH
        )
    pieces = tile_sem.shape[0]
    piece = slots // pieces
    tile_copies = [
        pltpu.make_async_copy(
            tiles.at[pl.ds(n * piece, piece)], held.at[pl.ds(n * piece, piece)], tile_sem.at[n]
        )
        for n in range(pieces)
    ]
    for copy in tile_copies:
        copy.start()

    for copy in index_copies:
        copy.wait()

    live_count = count[0]
    keys = [lax.div(quartet[0, t], row_blocks) * slots + t for t in range(slots)]

    def pick(u, previous):
        found = [jnp.where(key > previous, key, 1 << 30) for key in keys]
        while len(found) > 1:
            found = [jnp.minimum(a, b) for a, b in zip(found[::2], found[1::2])]
        t = lax.rem(found[0], slots)
        words = [quartet[n, t] for n in range(4)] + [jnp.where(t < live_count, 1, 0), t]
        for n, word in enumerate(words):
            meta_c[my_row, u * WORDS + n] = word
            meta_r[my_col, u * WORDS + n] = word
        return found[0]

    lax.fori_loop(0, slots, pick, jnp.int32(-1))
    for copy in dens_copies:
        copy.wait()
    for block_row in range(row_blocks):
        for chunk in range(chunks):
            rows = slice(block_row * SHELL, (block_row + 1) * SHELL)
            lanes = slice(chunk * LANES, (chunk + 1) * LANES)
            alpha, beta = dens_a[rows, lanes], dens_b[rows, lanes]
            at = block_row * chunks + chunk
            split_a[at], split_b[at] = alpha, beta
            summed[at] = (alpha.astype(F32) + beta.astype(F32)).astype(BF16)

    pl.semaphore_wait(barrier, n_row + n_col - 2)
    for step in range(n_row - 1, 0, -1):
        column_copy(0, meta_c.at[my_row], meta_c.at[my_row], row_peer(step), my_row).start()
    for step in range(1, n_col):
        row_copy(0, meta_r.at[my_col], meta_r.at[my_col], col_peer(step), my_col).start()

    group = iota((SHELL, LANES), 1) // SHELL

    fold_one = one_hot((LANES, LANES), lambda i, j: lax.rem(i, SHELL) == lax.rem(j, SHELL))

    def block_of(ref, block_row, block_col, mine):
        chunk = ref[block_row * chunks + lax.div(block_col, PACK)].astype(F32)
        inside = jnp.where(mine, lax.rem(block_col, PACK), -1)
        return jnp.where(group == inside, chunk, 0.0)

    def packed_blocks(blocks):
        spread_out = dot(jnp.concatenate(blocks, axis=0).astype(BF16), fold_one)
        halves = []
        for half in range(slots // PACK):
            total = jnp.zeros((SHELL, LANES), F32)
            for slot in range(PACK):
                first = (half * PACK + slot) * SHELL
                total = jnp.where(group == slot, spread_out[first : first + SHELL], total)
            halves.append(total)
        return jnp.concatenate(halves, axis=0).astype(BF16)

    def answer_column(source, target):
        blocks = []
        for slot in range(slots):
            s_at = meta_c[source, slot * WORDS + 3] - first_row
            r_at = jnp.clip(meta_c[source, slot * WORDS + 2] - first_col, 0, col_blocks - 1)
            mine = (s_at >= 0) & (s_at < row_blocks)
            blocks.append(block_of(summed, jnp.where(mine, s_at, 0), r_at, mine))
        target[source] = packed_blocks(blocks)

    def answer_row(source, target):
        blocks = [[], []]
        for slot in range(slots):
            q_at = jnp.clip(meta_r[source, slot * WORDS + 1] - first_row, 0, row_blocks - 1)
            s_at = meta_r[source, slot * WORDS + 3] - first_col
            mine = (s_at >= 0) & (s_at < col_blocks)
            s_at = jnp.where(mine, s_at, 0)
            for x, ref in enumerate((split_a, split_b)):
                blocks[x].append(block_of(ref, q_at, s_at, mine))
        half_rows = slots // PACK * SHELL
        for x in range(2):
            target[source, x * half_rows : (x + 1) * half_rows, :] = packed_blocks(blocks[x])

    answer_column(my_row, recv_c)
    answer_row(my_col, recv_r)

    def serve_row(step, carry):
        peer = col_peer(step)
        row_copy(0, meta_r.at[peer], meta_r.at[peer], peer, peer).wait_recv()
        answer_row(peer, send_r)
        row_copy(1, send_r.at[peer], recv_r.at[my_col], peer, my_col).start()
        return carry

    def serve_column(step, carry):
        peer = row_peer(step)
        column_copy(0, meta_c.at[peer], meta_c.at[peer], peer, peer).wait_recv()
        answer_column(peer, send_c)
        column_copy(1, send_c.at[peer], recv_c.at[my_row], peer, my_row).start()
        return carry

    lax.fori_loop(1, n_col, serve_row, 0)
    lax.fori_loop(1, n_row, serve_column, 0)

    def place_row(source, carry):
        for m in range(row_cap):
            base = (my_row * row_cap + m) * WORDS
            at = (source * row_cap + m) * 4
            place[at] = meta_c[source, base] - first_row
            place[at + 1] = meta_c[source, base + 2] - first_col
            place[at + 2] = meta_c[source, base + 4]
        return carry

    def place_col(source, carry):
        for m in range(col_cap):
            base = (my_col * col_cap + m) * WORDS
            at = (slots + source * col_cap + m) * 4
            place[at] = meta_r[source, base + 1] - first_row
            place[at + 1] = meta_r[source, base] - first_col
            place[at + 2] = meta_r[source, base + 4]
        return carry

    lax.fori_loop(0, n_row, place_row, 0)
    lax.fori_loop(0, n_col, place_col, 0)

    fold = one_hot((LANES, width), lambda i, j: lax.rem(i, SHELL) == lax.rem(j, SHELL))
    gather = one_hot((width, LANES), lambda i, j: lax.div(i, SHELL) == lax.rem(j, SHELL))
    pick_slot = [one_hot((LANES, LANES), lambda i, j: i // SHELL == slot) for slot in range(PACK)]
    shape = (SHELL * SHELL, LANES)
    own_r = iota(shape, 0) // SHELL == lax.rem(iota(shape, 1), SHELL)

    def expand(packed):
        return jnp.concatenate(
            [
                jnp.where(
                    group == t % PACK,
                    packed[(t // PACK) * SHELL : (t // PACK + 1) * SHELL],
                    0.0,
                )
                for t in range(slots)
            ],
            axis=0,
        ).astype(BF16)

    def arrive(count_of, copy_of, peer_of, ref):
        def wait(step, carry):
            copy_of(1, ref.at[peer_of(step)], ref.at[peer_of(step)], peer_of(step), peer_of(step)).wait_recv()
            return carry

        lax.fori_loop(1, count_of, wait, 0)
        total = ref[0].astype(F32)
        for n in range(1, count_of):
            total = total + ref[n].astype(F32)
        return total

    spins = arrive(n_col, row_copy, col_peer, recv_r)
    half_rows = (slots // PACK) * SHELL
    drep_a[...] = dot(expand(spins[:half_rows]), fold)
    drep_b[...] = dot(expand(spins[half_rows:]), fold)
    for copy in tile_copies:
        copy.wait()

    def exchange(t, carry):
        rows = pl.ds(pl.multiple_of(t * SHELL, SHELL), SHELL)
        tile = held[meta_c[my_row, t * WORDS + 5]].astype(F32).reshape(SHELL, SHELL, width)
        part_a[rows, :] = jnp.sum(tile * drep_a[rows, :][None], axis=1)
        part_b[rows, :] = jnp.sum(tile * drep_b[rows, :][None], axis=1)
        return carry

    lax.fori_loop(0, slots, exchange, 0)
    exch_a = dot_split(part_a[...], gather)
    exch_b = dot_split(part_b[...], gather)
    for k in range(n_row):
        total = jnp.zeros((SHELL, LANES), F32)
        for m in range(row_cap):
            first = (k * row_cap + m) * SHELL
            total = jnp.where(group == 2 * m, exch_a[first : first + SHELL], total)
            total = jnp.where(group == 2 * m + 1, exch_b[first : first + SHELL], total)
        xs[k] = total

    def send_x(step, carry):
        peer = row_peer(step)
        column_copy(2, xs.at[peer], xr.at[my_row], peer, my_row).start()
        return carry

    lax.fori_loop(1, n_row, send_x, 0)
    xr[my_row] = xs[my_row]

    coul = arrive(n_row, column_copy, row_peer, recv_c)
    for half in range(slots // PACK):
        block = coul[half * SHELL : (half + 1) * SHELL]
        stacked = jnp.concatenate([block] * SHELL, axis=0)
        column = jnp.where(own_r, stacked, 0.0).astype(BF16)
        for slot in range(PACK):
            weights[half * PACK + slot] = dot(column, pick_slot[slot]).astype(BF16)

    def coulomb(t, carry):
        out = dot(held[meta_c[my_row, t * WORDS + 5]], weights[t])
        blocks_j[t] = jnp.sum(jnp.where(own_r, out, 0.0).reshape(SHELL, SHELL, LANES), axis=0)
        return carry

    lax.fori_loop(0, slots, coulomb, 0, unroll=4)
    for k in range(n_col):
        total = jnp.zeros((SHELL, LANES), F32)
        for m in range(col_cap):
            total = jnp.where(group == m, blocks_j[k * col_cap + m], total)
        cs[k] = total

    def send_j(step, carry):
        peer = col_peer(step)
        row_copy(2, cs.at[peer], cr.at[my_col], peer, my_col).start()
        return carry

    lax.fori_loop(1, n_col, send_j, 0)
    cr[my_col] = cs[my_col]

    def finish_row(step, carry):
        peer = col_peer(step)
        row_copy(2, cs.at[peer], cr.at[peer], peer, peer).wait()
        row_copy(1, send_r.at[peer], recv_r.at[peer], peer, peer).wait_send()
        row_copy(0, meta_r.at[my_col], meta_r.at[my_col], peer, peer).wait_send()
        return carry

    def finish_column(step, carry):
        peer = row_peer(step)
        column_copy(2, xs.at[peer], xr.at[peer], peer, peer).wait()
        column_copy(1, send_c.at[peer], recv_c.at[peer], peer, peer).wait_send()
        column_copy(0, meta_c.at[my_row], meta_c.at[my_row], peer, peer).wait_send()
        return carry

    lax.fori_loop(1, n_row, finish_column, 0)
    lax.fori_loop(1, n_col, finish_row, 0)
    out_x[...] = xr[...]
    out_c[...] = cr[...]


def place_kernel(place, in_x, in_c, out_a, out_b):
    n_row, n_col = in_x.shape[0], in_c.shape[0]
    slots = place.shape[0] // 8
    row_cap, col_cap = slots // n_row, slots // n_col
    out_a[...] = jnp.zeros_like(out_a)
    out_b[...] = jnp.zeros_like(out_b)
    group = iota((SHELL, LANES), 1) // SHELL

    def where_to(at):
        block_col = place[at + 1]
        rows = pl.ds(pl.multiple_of(place[at] * SHELL, SHELL), SHELL)
        lanes = pl.ds(pl.multiple_of(lax.div(block_col, PACK) * LANES, LANES), LANES)
        inside = lax.rem(block_col, PACK)
        return rows, lanes, inside, group == jnp.where(place[at + 2] != 0, inside, -1)

    def moved(block, here, inside, mask):
        shift = lax.rem(inside - here + PACK, PACK) * SHELL
        return jnp.where(mask, pltpu.roll(block, shift, 1), 0.0)

    for source in range(n_col):
        block = in_c[source]
        for m in range(col_cap):
            rows, lanes, inside, mask = where_to((slots + source * col_cap + m) * 4)
            value = moved(block, m, inside, mask)
            out_a[rows, lanes] += value
            out_b[rows, lanes] += value
    for source in range(n_row):
        block = in_x[source]
        for m in range(row_cap):
            rows, lanes, inside, mask = where_to((source * row_cap + m) * 4)
            out_a[rows, lanes] -= moved(block, 2 * m, inside, mask)
            out_b[rows, lanes] -= moved(block, 2 * m + 1, inside, mask)


def local(n_row, n_col, dens_alpha, dens_beta, integrals, tile_quartet, tile_count):
    slots, width = integrals.shape[0], integrals.shape[1]
    vmem = pl.BlockSpec(memory_space=pltpu.VMEM)
    smem = pl.BlockSpec(memory_space=pltpu.SMEM)
    hbm = pl.BlockSpec(memory_space=pltpu.HBM)
    rows = slots * SHELL
    pack_rows = slots // PACK * SHELL
    meta_words = max(LANES, slots * WORDS)
    split = pltpu.VMEM((dens_alpha.size // (SHELL * LANES), SHELL, LANES), BF16)
    blocks_x, blocks_c, place = pl.pallas_call(
        functools.partial(build_kernel, n_row, n_col),
        out_shape=(
            jax.ShapeDtypeStruct((n_row, SHELL, LANES), F32),
            jax.ShapeDtypeStruct((n_col, SHELL, LANES), F32),
            jax.ShapeDtypeStruct((slots * 8,), jnp.int32),
        ),
        in_specs=[hbm] * 5,
        out_specs=(vmem, vmem, smem),
        scratch_shapes=[
            pltpu.SMEM((4, slots), jnp.int32),
            pltpu.SMEM((1,), jnp.int32),
            pltpu.VMEM(dens_alpha.shape, BF16),
            pltpu.VMEM(dens_alpha.shape, BF16),
            pltpu.SMEM((n_row, meta_words), jnp.int32),
            pltpu.SMEM((n_col, meta_words), jnp.int32),
            split,
            split,
            split,
            pltpu.VMEM(integrals.shape, BF16),
            pltpu.VMEM((n_row, pack_rows, LANES), BF16),
            pltpu.VMEM((n_row, pack_rows, LANES), BF16),
            pltpu.VMEM((n_col, 2 * pack_rows, LANES), BF16),
            pltpu.VMEM((n_col, 2 * pack_rows, LANES), BF16),
            pltpu.VMEM((rows, width), F32),
            pltpu.VMEM((rows, width), F32),
            pltpu.VMEM((slots, width, LANES), BF16),
            pltpu.VMEM((rows, width), F32),
            pltpu.VMEM((rows, width), F32),
            pltpu.VMEM((slots, SHELL, LANES), F32),
            pltpu.VMEM((n_row, SHELL, LANES), F32),
            pltpu.VMEM((n_row, SHELL, LANES), F32),
            pltpu.VMEM((n_col, SHELL, LANES), F32),
            pltpu.VMEM((n_col, SHELL, LANES), F32),
            pltpu.SemaphoreType.DMA((2,)),
            pltpu.SemaphoreType.DMA((2,)),
            pltpu.SemaphoreType.DMA((4,)),
            pltpu.SemaphoreType.DMA((3, n_row)),
            pltpu.SemaphoreType.DMA((3, n_row)),
            pltpu.SemaphoreType.DMA((3, n_col)),
            pltpu.SemaphoreType.DMA((3, n_col)),
        ],
        compiler_params=pltpu.CompilerParams(collective_id=0, has_side_effects=True),
        name="build",
    )(tile_quartet.T, tile_count, dens_alpha, dens_beta, integrals)
    out = jax.ShapeDtypeStruct(dens_alpha.shape, F32)
    return pl.pallas_call(
        place_kernel,
        out_shape=(out, out),
        in_specs=[smem, vmem, vmem],
        out_specs=(vmem, vmem),
        name="place",
    )(place, blocks_x, blocks_c)


def solution(mesh):
    in_specs = (
        P("row", "col"),
        P("row", "col"),
        P(("row", "col"), None, None),
        P(("row", "col"), None),
        P(("row", "col")),
    )
    body = functools.partial(local, mesh.shape["row"], mesh.shape["col"])
    return jax.shard_map(
        body, mesh=mesh, in_specs=in_specs, out_specs=(P("row", "col"), P("row", "col")),
        check_vma=False,
    )
```
